32 devices in a mesh: group: 4 (over x, core), shard: 8 (over z, y).
Axes of the slice: x: 2, y: 2, z: 4, core: 2. Of those that a mesh axis runs over, the one named last changes fastest.
Arguments:
- step_index: int32 [1], replicated, may hold values from 0 to 1023
- hidden: bfloat16 [4, 8192, 4608], P('group', 'shard'), may hold values from -600 to 600
- upstream: bfloat16 [4, 8192, 2304], P('group', 'shard'), may hold values from -40 to 40
- numerator: float32 [4, 4608, 2304], P('group', 'shard'), may hold values from -6 to 6
- push_weight: float32 [4], P('group'), may hold values from 0.5 to 2
Outputs:
- numerator_next: float32 [4, 4608, 2304], P('group', 'shard')
- weight_next: float32 [4], P('group')
- params: bfloat16 [4, 4608, 2304], P('group', 'shard')
The draws below stay inside these ranges and needn't reach their ends.
All inputs are finite; a program needn't handle non-finite values.
Results may differ from the reference program's by a relative error of at most 0.009.
Values may be sent and summed in bfloat16 or wider, within the bound.
A program may use at most 128 MiB of HBM per device.

```python
import math
import jax
import jax.numpy as jnp
from jax import lax

D = 2304
FF = 4608
TOK_DEV = 1024
GROUPS = 4
SHARDS = 8
TOK_GROUP = 8192


def draw_hidden(key, part):
    keys = jax.random.split(key, 4)
    position = jnp.arange(FF, dtype=jnp.float32)
    column_scale = 10.0 ** jax.random.uniform(keys[0], (FF,), jnp.float32) * 3.0 ** (position / FF) / 4.0
    row_scale = 10.0 ** jax.random.uniform(keys[1], (GROUPS, TOK_GROUP, 1), jnp.float32) / 4.0
    owner = jax.random.permutation(keys[2], SHARDS)
    token_block = jnp.arange(TOK_GROUP) // TOK_DEV
    unit_block = jnp.arange(FF) // (FF // SHARDS)
    spike = jnp.where(owner[token_block][:, None] == unit_block[None, :], 3.0, 1.0)
    shape = (GROUPS, TOK_GROUP, FF)
    base = jnp.clip(jax.random.normal(keys[3], shape, jnp.float32), -5.0, 5.0)
    return (base * row_scale * column_scale * spike).astype(jnp.bfloat16)


def draw_upstream(key, part):
    keys = jax.random.split(key, 2)
    column_scale = 10.0 ** jax.random.uniform(keys[0], (D,), jnp.float32) / 3.0
    shape = (GROUPS, TOK_GROUP, D)
    base = jnp.clip(jax.random.normal(keys[1], shape, jnp.float32), -5.0, 5.0)
    return (base * column_scale).astype(jnp.bfloat16)


def steps_of(stream_key, shape, shards, smallest, high):
    gain, own = 1.0, jax.random.fold_in(stream_key, 6)
    for axis_at, parts in shards:
        heights = jnp.exp(jax.random.uniform(jax.random.fold_in(own, axis_at), (parts,), jnp.float32, smallest / len(shards), high / len(shards)))
        gain = gain * jnp.repeat(heights, shape[axis_at] // parts).reshape([-1 if axis == axis_at else 1 for axis in range(len(shape))])
    return gain


def scatter_about(own_key, dims, scale, bound, cuts=(), held_as=jnp.bfloat16):
    level = steps_of(own_key, dims, cuts, -0.22, 0.18) if cuts else 1.0
    result = jax.random.normal(own_key, dims, jnp.float32) * scale * level
    return jnp.minimum(jnp.maximum(result, -bound), bound).astype(held_as)


def setup_inputs(seed: int = 0) -> dict:
    splits = jax.random.split(jax.random.key(seed), 6)
    return {
        "step_index": jax.random.randint(splits[0], (1,), 0, 1024).astype(jnp.int32),
        "hidden": draw_hidden(jax.random.fold_in(splits[5], 71), 0),
        "upstream": draw_upstream(jax.random.fold_in(splits[5], 71), 0),
        "numerator": scatter_about(splits[3], (GROUPS, FF, D), 1.0, 6.0, ((0, 4), (1, 8)), jnp.float32),
        "push_weight": jnp.clip(jnp.exp(math.log(2.0) - 1.3862944 * jax.random.uniform(splits[4], (GROUPS,), jnp.float32) ** steps_of(splits[4], (GROUPS,), ((0, 4),), -0.2, 0.2)), 0.5, 2.0),
    }


learning_rate = 0.3
decay_steps = 256.0
clip_ceiling = 1.0
epsilon = 1e-06

def shard_gradient(hidden_rows, upstream_rows):
    hidden_blocks = hidden_rows.reshape(SHARDS, TOK_DEV, FF)
    upstream_blocks = upstream_rows.reshape(SHARDS, TOK_DEV, D)

    def accumulate(running, shard_pair):
        product = jnp.dot(shard_pair[0].astype(jnp.float32).T, shard_pair[1].astype(jnp.float32), preferred_element_type=jnp.float32, precision=lax.Precision.HIGHEST)
        rounded = lax.optimization_barrier(product.astype(jnp.bfloat16))
        return (running + rounded.astype(jnp.float32), None)
    summed, unused = lax.scan(accumulate, jnp.zeros((FF, D), jnp.float32), (hidden_blocks, upstream_blocks))
    return summed

def group_pair(arrays):
    return shard_gradient(arrays[0], arrays[1])

def reference(step_index, hidden, upstream, numerator, push_weight):
    gradient = lax.map(group_pair, (hidden, upstream))
    square_mean = lax.optimization_barrier(jnp.sum(gradient * gradient, axis=(1, 2))) / (FF * D)
    rate = learning_rate / jnp.sqrt(1.0 + step_index[0].astype(jnp.float32) / decay_steps)
    factor = rate * jnp.minimum(1.0, clip_ceiling / jnp.sqrt(square_mean + epsilon))
    pushed = numerator - factor[:, None, None] * gradient
    level_count = GROUPS.bit_length() - 1
    exponent = (step_index[0] % level_count).astype(jnp.int32)
    offset = jnp.left_shift(jnp.int32(1), exponent)
    peer_state = jnp.roll(pushed, offset, axis=0)
    peer_weight = jnp.roll(push_weight, offset, axis=0)
    numerator_next = 0.5 * (pushed + peer_state)
    weight_next = 0.5 * (push_weight + peer_weight)
    params = (numerator_next / weight_next[:, None, None]).astype(jnp.bfloat16)
    return (numerator_next, weight_next, params)
```

```python
import functools

import jax
import jax.numpy as jnp
from jax import lax
from jax.experimental import pallas as pl
from jax.experimental.pallas import tpu as pltpu
from jax.sharding import PartitionSpec as P

learning_rate = 0.3
decay_steps = 256.0
clip_ceiling = 1.0
epsilon = 1e-06
LANES = 128
LINKED = jnp.bfloat16
MESH = pl.DeviceIdType.MESH
NEAR = 2
AHEAD = 3
RING = 4
FLIGHT = 2


def wide(x):
    return x.astype(jnp.float32)


def step_of_rows(rows):
    for step in (96, 64, 48, 32, 16):
        if rows % step == 0:
            return step
    return rows


def kernel(plan, hidden, upstream, state, weight, grad, totals, peer_states, peer_grads, *refs):
    groups, far, near, rows, offsets = (plan[k] for k in ("groups", "far", "near", "rows", "offsets"))
    first, pieces, splits, tile = (plan[k] for k in ("first", "pieces", "splits", "tile"))
    levels, count, half = len(offsets), far * near, rows // splits
    (units, cotangent, own, away, came, slots, first_own, first_slots, turn_own, turn_out, turn_in, cast, stage,
     running, norms, fetch_sem, stage_sem, near_send, near_recv, up_send, up_recv, down_send, down_recv,
     first_up_send, first_up_recv, first_down_send, first_down_recv, turn_send, turn_recv, state_send, state_recv,
     grad_send, grad_recv, norm_send, norm_recv) = refs

    g, s = lax.axis_index("group"), lax.axis_index("shard")
    z, y = s // near, s % near
    near_peer = (g, z * near + (near - 1 - y))
    above = (g, (s + near) % count)
    below = (g, (s + count - near) % count)
    chunks, blocks = far * near * rows // tile, tile // (near * rows)
    chunk_rows = stage.shape[1]

    receivers = [(0, d) for d in range(1, count)]
    receivers += [(d, e) for d in range(1, groups) for e in range(count)]
    barrier = pltpu.get_barrier_semaphore()
    for d, e in receivers:
        pl.semaphore_signal(barrier, inc=1, device_id=((g + d) % groups, (s + e) % count), device_id_type=MESH)

    def remote(src, dst, send, recv, device):
        return pltpu.make_async_remote_copy(
            src_ref=src, dst_ref=dst, send_sem=send, recv_sem=recv, device_id=device, device_id_type=MESH
        )

    def part(h):
        return pl.ds(h * half, half)

    def columns(at, size=LANES):
        return pl.ds(pl.multiple_of(at * LANES, LANES), size)

    def near_copy(c, h):
        return remote(
            away.at[c % RING, :, part(h)], came.at[c, :, part(h)], near_send.at[c, h], near_recv.at[c, h], near_peer
        )

    def up_copy(c, h, t, b):
        at = slots.at[c, b, part(h)]
        return remote(at, at, up_send.at[c, h, t], up_recv.at[c, h, t], above)

    def down_copy(c, h, t, b):
        to = jnp.where(t == far - 2, far, b)
        return remote(
            slots.at[c, b, part(h)], slots.at[c, to, part(h)], down_send.at[c, h, t], down_recv.at[c, h, t], below
        )

    def first_up_copy(j, t, b):
        at = first_slots.at[j, b]
        return remote(at, at, first_up_send.at[j, t], first_up_recv.at[j, t], above)

    def first_down_copy(j, t, b):
        to = jnp.where(t == far - 2, far, b)
        return remote(
            first_slots.at[j, b], first_slots.at[j, to], first_down_send.at[j, t], first_down_recv.at[j, t], below
        )

    def turn_copy(j):
        return remote(turn_out.at[j], turn_in.at[j], turn_send.at[j], turn_recv.at[j], near_peer)

    def state_copy(l):
        return remote(cast, peer_states.at[l], state_send.at[l], state_recv.at[l], ((g + offsets[l]) % groups, s))

    def grad_copy(at, h, l):
        return remote(
            grad.at[part(h), columns(at)],
            peer_grads.at[l, part(h), columns(at)],
            grad_send.at[at, h, l],
            grad_recv.at[at, h, l],
            ((g + offsets[l]) % groups, s),
        )

    def each_rows(body):
        step = step_of_rows(rows)

        def once(i, carry):
            body(pl.ds(pl.multiple_of(i * step, step), step))
            return carry

        lax.fori_loop(0, rows // step, once, 0)

    def loop(low, high, body):
        def once(i, carry):
            body(i)
            return carry

        lax.fori_loop(low, high, once, 0)

    def fetch_units(k):
        at = pl.ds(pl.multiple_of(k * tile, tile), tile)
        return pltpu.make_async_copy(hidden.at[:, at], units.at[:, at], fetch_sem.at[k])

    def fetch_cotangent(i, low, high):
        at = pl.ds(low * LANES, (high - low) * LANES)
        return pltpu.make_async_copy(upstream.at[:, at], cotangent.at[:, at], fetch_sem.at[chunks + i])

    def compute(at, places, loading=False):
        size = len(places) * LANES

        def once(k):
            if loading:
                fetch_units(k).wait()
            product = lax.dot_general(
                units[:, pl.ds(pl.multiple_of(k * tile, tile), tile)],
                cotangent[:, columns(at, size)],
                (((0,), (0,)), ((), ())),
                preferred_element_type=jnp.float32,
            ).reshape(blocks, near, rows, size)
            to = pl.ds(k * blocks, blocks)
            for i, (kind, index) in enumerate(places):
                piece = product[:, :, :, i * LANES : (i + 1) * LANES]
                if kind == "first":
                    first_own[index, to] = piece.astype(LINKED)
                else:
                    own[index, to] = jnp.where(y == 0, piece[:, 0], piece[:, 1]).astype(LINKED)
                    away[index % RING, to] = jnp.where(y == 0, piece[:, 1], piece[:, 0]).astype(LINKED)

        loop(0, chunks, once)

    def line(t, edge, middle, fill, up, down):
        up_b = far - 1 - t + z
        down_b = t - (far - 1) + z
        if edge:
            @pl.when(z == 0)
            def _():
                fill(up_b, False)
                up(t, up_b).start()

            @pl.when(z == far - 1)
            def _():
                fill(down_b, False)
                down(t, down_b).start()

        if middle:
            @pl.when((z > 0) & (z <= t) & (z < far - 1))
            def _():
                up(t - 1, up_b).wait_recv()
                fill(up_b, True)
                up(t, up_b).start()

            @pl.when((z < far - 1) & (z >= far - 1 - t) & (z > 0))
            def _():
                down(t - 1, down_b).wait_recv()
                fill(down_b, True)
                down(t, down_b).start()

    def term(c, h, b):
        return wide(own[c, b, part(h), :]) + wide(came[c, b, part(h), :])

    def line_step(c, h, t):
        def fill(b, add):
            value = term(c, h, b)
            if add:
                value = value + wide(slots[c, b, part(h), :])
            slots[c, b, part(h), :] = value.astype(LINKED)

        line(t, True, True, fill, lambda t, b: up_copy(c, h, t, b), lambda t, b: down_copy(c, h, t, b))

    def first_step(j, t, edge, middle):
        def fill(b, add):
            for side in range(near):
                def body(r):
                    value = first_own[j, b, side, r, :]
                    if add:
                        value = (wide(value) + wide(first_slots[j, b, side, r, :])).astype(LINKED)
                    first_slots[j, b, side, r, :] = value

                each_rows(body)

        line(t, edge, middle, fill, lambda t, b: first_up_copy(j, t, b), lambda t, b: first_down_copy(j, t, b))

    def settle(at, h, value):
        grad[part(h), columns(at)] = value.astype(LINKED)
        square = value * value
        total = square[0:8]
        for i in range(8, half, 8):
            total = total + square[i : i + 8]
        running[0] = running[0] + total
        for l in range(levels):
            grad_copy(at, h, l).start()

    def wait_own(up, down):
        @pl.when(z > 0)
        def _():
            up(far - 2, z).wait_recv()

        @pl.when(z < far - 1)
        def _():
            down(far - 2, far).wait_recv()

    def finish(c, h):
        wait_own(lambda t, b: up_copy(c, h, t, b), lambda t, b: down_copy(c, h, t, b))
        value = term(c, h, z)
        value = value + jnp.where(z > 0, wide(slots[c, z, part(h), :]), 0.0)
        value = value + jnp.where(z < far - 1, wide(slots[c, far, part(h), :]), 0.0)
        settle(first + c, h, value)

    def finish_first(j):
        wait_own(lambda t, b: first_up_copy(j, t, b), lambda t, b: first_down_copy(j, t, b))

        def put(r):
            def own_value(side):
                value = wide(first_own[j, z, side, r, :])
                value = value + jnp.where(z > 0, wide(first_slots[j, z, side, r, :]), 0.0)
                return value + jnp.where(z < far - 1, wide(first_slots[j, far, side, r, :]), 0.0)

            turn_own[j, r, :] = own_value(y)
            turn_out[j, r, :] = own_value(near - 1 - y).astype(LINKED)

        each_rows(put)
        turn_copy(j).start()

    def finish_turn(j):
        turn_copy(j).wait()
        for h in range(splits):
            settle(first - 1 - j, h, turn_own[j, part(h), :] + wide(turn_in[j, part(h), :]))

    steps = first * (far - 1)
    span = max(1, pieces - 3)

    def reached(c):
        goal = far - 1 + lax.div((c + 1) * (steps - (far - 1)), span)
        return jnp.where(c < 0, 0, jnp.minimum(steps, goal))

    def when(condition, body):
        pl.when(condition)(body)

    lead = (first - 1, first + 1)
    fetch_cotangent(0, *lead).start()
    loop(0, chunks, lambda k: fetch_units(k).start())
    fetch_cotangent(1, lead[1], first + pieces).start()
    fetch_cotangent(2, 0, lead[0]).start()
    running[0] = jnp.zeros((8, LANES), jnp.float32)
    running[1] = weight[...]
    fetch_cotangent(0, *lead).wait()
    compute(first - 1, [("first", 0), ("near", 0)], loading=True)
    pl.semaphore_wait(barrier, len(receivers))
    for k in range(FLIGHT):
        near_copy(k // splits, k % splits).start()
    loop(0, far - 1, lambda t: first_step(0, t, True, False))
    fetch_cotangent(1, lead[1], first + pieces).wait()
    fetch_cotangent(2, 0, lead[0]).wait()
    compute(first + 1, [("near", c) for c in range(1, AHEAD)])
    compute(0, [("first", j) for j in range(first - 1, 0, -1)])

    def stage_copy(i):
        return pltpu.make_async_copy(
            state.at[pl.ds(pl.multiple_of(i * chunk_rows, chunk_rows), chunk_rows)], stage.at[i % 2], stage_sem.at[i % 2]
        )

    stage_copy(0).start()

    def cast_rows(i):
        stage_copy(i).wait()
        when(i + 1 < rows // chunk_rows, lambda: stage_copy(i + 1).start())
        cast[pl.ds(pl.multiple_of(i * chunk_rows, chunk_rows), chunk_rows), :] = stage[i % 2].astype(LINKED)

    loop(0, rows // chunk_rows, cast_rows)
    for l in range(levels):
        state_copy(l).start()

    def prepare(c):
        for h in range(splits):
            when(c >= RING, lambda: near_copy(c - RING, h).wait_send())
        compute(first + c, [("near", c)])

    def tick(c):
        for h in range(splits):
            done = c - (far - 1)
            when((done >= 0) & (done < pieces), lambda: finish(done, h))

            def older(i):
                t = far - 2 - i
                when((c - t >= 0) & (c - t < pieces), lambda: line_step(c - t, h, t))

            loop(0, far - 2, older)

            @pl.when(c < pieces)
            def _():
                near_copy(c, h).wait_recv()
                later = c + (h + FLIGHT) // splits
                when(later < pieces, lambda: near_copy(later, (h + FLIGHT) % splits).start())
                line_step(c, h, 0)

            if h == 0:
                when(c + AHEAD < pieces, lambda: prepare(c + AHEAD))
        loop(lax.div(reached(c - 3), far - 1), lax.div(reached(c - 2), far - 1), finish_turn)
        loop(lax.div(reached(c - 2), far - 1), lax.div(reached(c - 1), far - 1), finish_first)

        def first_at(q):
            j, t = lax.div(q, far - 1), lax.rem(q, far - 1)
            when(j > 0, lambda: first_step(j, t, True, False))
            first_step(j, t, False, True)

        loop(reached(c - 1), reached(c), first_at)

    loop(0, pieces + far - 1, tick)

    def norm_copy(l, s_from, e):
        d = 0 if l == 0 else offsets[l - 1]
        at = norms.at[l, s_from]
        return remote(running, at, norm_send.at[l, e], norm_recv.at[l, e], ((g + d) % groups, (s + e) % count))

    messages = [(l, e) for l in range(levels + 1) for e in range(count) if l or e]
    for l, e in messages:
        norm_copy(l, s, e).start()
    norms[0, s] = running[...]
    for l, e in messages:
        norm_copy(l, (s + count - e) % count, e).wait_recv()
    for l in range(levels + 1):
        total = norms[l, 0, 0]
        for d in range(1, count):
            total = total + norms[l, d, 0]
        totals[l, 0] = total
        totals[l, 1] = norms[l, 0, 1]

    for l, e in messages:
        norm_copy(l, s, e).wait_send()

    def drain_line(t, up, down):
        @pl.when((z <= t) & (z < far - 1))
        def _():
            up(t, far - 1 - t + z).wait_send()

        @pl.when((z >= far - 1 - t) & (z > 0))
        def _():
            down(t, t - (far - 1) + z).wait_send()

    def drain(c):
        for h in range(splits):
            when(c >= pieces - RING, lambda: near_copy(c, h).wait_send())
            loop(0, far - 1, lambda t: drain_line(
                t, lambda t, b: up_copy(c, h, t, b), lambda t, b: down_copy(c, h, t, b)))

    def drain_first(j):
        loop(0, far - 1, lambda t: drain_line(
            t, lambda t, b: first_up_copy(j, t, b), lambda t, b: first_down_copy(j, t, b)))

    def drain_grads(at):
        for h in range(splits):
            for l in range(levels):
                grad_copy(at, h, l).wait()

    loop(0, pieces, drain)
    loop(0, first, drain_first)
    loop(0, first + pieces, drain_grads)
    for l in range(levels):
        state_copy(l).wait()


def reduced(hidden, upstream, state, weight, plan):
    far, near, rows, first, pieces, splits = (plan[k] for k in ("far", "near", "rows", "first", "pieces", "splits"))
    levels, count, width = len(plan["offsets"]), far * near, state.shape[1]
    anywhere, vmem = pl.BlockSpec(memory_space=pl.ANY), pl.BlockSpec(memory_space=pltpu.VMEM)
    dma, single = pltpu.SemaphoreType.DMA, jnp.float32
    scratch = [
        pltpu.VMEM(hidden.shape, LINKED),
        pltpu.VMEM(upstream.shape, LINKED),
        pltpu.VMEM((pieces, far, rows, LANES), LINKED),
        pltpu.VMEM((RING, far, rows, LANES), LINKED),
        pltpu.VMEM((pieces, far, rows, LANES), LINKED),
        pltpu.VMEM((pieces, far + 1, rows, LANES), LINKED),
        pltpu.VMEM((first, far, near, rows, LANES), LINKED),
        pltpu.VMEM((first, far + 1, near, rows, LANES), LINKED),
        pltpu.VMEM((first, rows, LANES), single),
        pltpu.VMEM((first, rows, LANES), LINKED),
        pltpu.VMEM((first, rows, LANES), LINKED),
        pltpu.VMEM((rows, width), LINKED),
        pltpu.VMEM((2, step_of_rows(rows), width), single),
        pltpu.VMEM((2, 8, LANES), single),
        pltpu.VMEM((levels + 1, count, 2, 8, LANES), single),
        dma((far * near * rows // plan["tile"] + 3,)),
        dma((2,)),
    ]
    scratch += [dma((pieces, splits))] * 2 + [dma((pieces, splits, far - 1))] * 4 + [dma((first, far - 1))] * 4
    scratch += [dma((first,))] * 2 + [dma((levels,))] * 2 + [dma((first + pieces, splits, levels))] * 2
    scratch += [dma((levels + 1, count))] * 2
    peers = jax.ShapeDtypeStruct((levels, rows, width), LINKED)
    return pl.pallas_call(
        functools.partial(kernel, plan),
        out_shape=[
            jax.ShapeDtypeStruct((rows, width), LINKED),
            jax.ShapeDtypeStruct((levels + 1, 2, 8, LANES), single),
            peers,
            peers,
        ],
        in_specs=[anywhere] * 3 + [vmem],
        out_specs=[vmem, vmem, anywhere, anywhere],
        scratch_shapes=scratch,
        compiler_params=pltpu.CompilerParams(
            collective_id=0, has_side_effects=True, vmem_limit_bytes=63 * 1024 * 1024
        ),
    )(hidden, upstream, state, weight)


def update(levels, entry_count, step, totals, state, grad, peer_state, peer_grad, mixed_out, params_out, weight_out):
    bit = lax.rem(step[0], levels)
    rate = learning_rate / jnp.sqrt(1.0 + jnp.full((8, LANES), step[0], jnp.int32).astype(jnp.float32) / decay_steps)

    def factor(l):
        squares = jnp.sum(totals[l, 0], keepdims=True)
        return (rate * jnp.minimum(1.0, clip_ceiling / jnp.sqrt(squares / entry_count + epsilon)))[0:1, 0:1]

    mine, other = factor(0), factor(1 + bit)
    weight_next = 0.5 * (totals[0, 1] + totals[1 + bit, 1])
    weight_out[0] = jnp.max(weight_next)
    pushed = state[...] - mine * wide(grad[...])
    came = wide(peer_state[0]) - other * wide(peer_grad[0])
    mixed = 0.5 * (pushed + came)
    mixed_out[...] = mixed
    params_out[...] = (mixed * (1.0 / weight_next)[0:1, 0:1]).astype(jnp.bfloat16)


def updated(step_index, totals, state, grad, peer_states, peer_grads, entry_count):
    levels, (rows, width) = peer_states.shape[0], state.shape
    step = step_of_rows(rows)
    here = pl.BlockSpec((step, width), lambda i, at: (i, 0))
    chosen = pl.BlockSpec((1, step, width), lambda i, at: (lax.rem(at[0], levels), i, 0))
    return pl.pallas_call(
        functools.partial(update, levels, entry_count),
        out_shape=[
            jax.ShapeDtypeStruct((rows, width), jnp.float32),
            jax.ShapeDtypeStruct((rows, width), jnp.bfloat16),
            jax.ShapeDtypeStruct((1,), jnp.float32),
        ],
        grid_spec=pltpu.PrefetchScalarGridSpec(
            num_scalar_prefetch=1,
            grid=(rows // step,),
            in_specs=[pl.BlockSpec(totals.shape, lambda i, at: (0, 0, 0, 0)), here, here, chosen, chosen],
            out_specs=[here, here, pl.BlockSpec(memory_space=pltpu.SMEM)],
        ),
    )(step_index, totals, state, grad, peer_states, peer_grads)


def shards(step_index, hidden, upstream, numerator, push_weight):
    own_state = numerator[0]
    groups = lax.axis_size("group")
    count = lax.axis_size("shard")
    level_count = groups.bit_length() - 1
    rows, width = own_state.shape
    units = rows * count
    tiles = width // LANES
    first = max(1, tiles // 6)
    plan = {
        "groups": groups,
        "far": count // NEAR,
        "near": NEAR,
        "rows": rows,
        "first": first,
        "pieces": tiles - first,
        "splits": 2 if rows % 32 == 0 else 1,
        "tile": next(t for t in (1152, units) if units % t == 0 and t % (NEAR * rows) == 0),
        "offsets": tuple(1 << bit for bit in range(level_count)),
    }
    weight = jnp.broadcast_to(push_weight[0], (8, LANES))
    gradient, totals, peer_states, peer_grads = reduced(hidden[0], upstream[0], own_state, weight, plan)
    mixed_state, new_params, weight_next = updated(
        step_index, totals, own_state, gradient, peer_states, peer_grads, units * width
    )
    return (mixed_state[None], weight_next, new_params[None])


def solution(mesh):
    placed = (
        P(),
        P("group", "shard", None),
        P("group", "shard", None),
        P("group", "shard", None),
        P("group"),
    )
    return jax.shard_map(
        shards,
        mesh=mesh,
        in_specs=placed,
        out_specs=(P("group", "shard", None), P("group"), P("group", "shard", None)),
        check_vma=False,
    )
```

```python
import functools

import jax
import jax.numpy as jnp
from jax import lax
from jax.experimental import pallas as pl
from jax.experimental.pallas import tpu as pltpu
from jax.sharding import PartitionSpec as P

learning_rate = 0.3
decay_steps = 256.0
clip_ceiling = 1.0
epsilon = 1e-06
LANES = 128
LINKED = jnp.bfloat16
MESH = pl.DeviceIdType.MESH
NEAR = 2
AHEAD = 3
RING = 4
FLIGHT = 2
EDGE = 1
MIDDLE = 2
START = 2
LAG = 1
DRAIN = 10
UPDATE = 144


def wide(x):
    return x.astype(jnp.float32)


def step_of_rows(rows):
    for step in (96, 64, 48, 32, 16):
        if rows % step == 0:
            return step
    return rows


def kernel(plan, hidden, upstream, state, weight, grad, totals, peer_states, peer_grads, *refs):
    groups, far, near, rows, offsets = (plan[k] for k in ("groups", "far", "near", "rows", "offsets"))
    first, pieces, splits, tile = (plan[k] for k in ("first", "pieces", "splits", "tile"))
    levels, count, half = len(offsets), far * near, rows // splits
    (units, cotangent, own, away, came, slots, first_own, first_slots, turn_own, turn_out, turn_in, cast, stage,
     running, summed, weights, norms, fetch_sem, stage_sem, near_send, near_recv, up_send, up_recv, down_send, down_recv,
     first_up_send, first_up_recv, first_down_send, first_down_recv, turn_send, turn_recv, state_send, state_recv,
     grad_send, grad_recv, norm_send, norm_recv, weight_send, weight_recv) = refs

    g, s = lax.axis_index("group"), lax.axis_index("shard")
    z, y = s // near, s % near
    near_peer = (g, z * near + (near - 1 - y))
    above = (g, (s + near) % count)
    below = (g, (s + count - near) % count)
    chunks, blocks = far * near * rows // tile, tile // (near * rows)
    chunk_rows = stage.shape[1]

    receivers = [(0, d) for d in range(1, count)]
    receivers += [(d, e) for d in range(1, groups) for e in range(count)]
    barrier = pltpu.get_barrier_semaphore()
    for d, e in receivers:
        pl.semaphore_signal(barrier, inc=1, device_id=((g + d) % groups, (s + e) % count), device_id_type=MESH)

    def remote(src, dst, send, recv, device):
        return pltpu.make_async_remote_copy(
            src_ref=src, dst_ref=dst, send_sem=send, recv_sem=recv, device_id=device, device_id_type=MESH
        )

    def part(h):
        return pl.ds(h * half if isinstance(h, int) else pl.multiple_of(h * half, half), half)

    def columns(at, size=LANES):
        return pl.ds(pl.multiple_of(at * LANES, LANES), size)

    def near_copy(c, h):
        return remote(
            away.at[c % RING, :, part(h)], came.at[c, :, part(h)], near_send.at[c, h], near_recv.at[c, h], near_peer
        )

    def up_copy(c, h, t, b):
        at = slots.at[c, b, part(h)]
        return remote(at, at, up_send.at[c, h, t], up_recv.at[c, h, t], above)

    def down_copy(c, h, t, b):
        to = jnp.where(t == far - 2, far, b)
        return remote(
            slots.at[c, b, part(h)], slots.at[c, to, part(h)], down_send.at[c, h, t], down_recv.at[c, h, t], below
        )

    def first_up_copy(j, t, b):
        at = first_slots.at[j, b]
        return remote(at, at, first_up_send.at[j, t], first_up_recv.at[j, t], above)

    def first_down_copy(j, t, b):
        to = jnp.where(t == far - 2, far, b)
        return remote(
            first_slots.at[j, b], first_slots.at[j, to], first_down_send.at[j, t], first_down_recv.at[j, t], below
        )

    def turn_copy(j):
        return remote(turn_out.at[j], turn_in.at[j], turn_send.at[j], turn_recv.at[j], near_peer)

    def state_copy(l):
        return remote(cast, peer_states.at[l], state_send.at[l], state_recv.at[l], ((g + offsets[l]) % groups, s))

    def weight_copy(l):
        to = weights.at[l + 1]
        return remote(weight, to, weight_send.at[l], weight_recv.at[l], ((g + offsets[l]) % groups, s))

    def grad_copy(at, h, l):
        return remote(
            grad.at[part(h), columns(at)],
            peer_grads.at[l, part(h), columns(at)],
            grad_send.at[at, h, l],
            grad_recv.at[at, h, l],
            ((g + offsets[l]) % groups, s),
        )

    def each_rows(body):
        step = step_of_rows(rows)

        def once(i, carry):
            body(pl.ds(pl.multiple_of(i * step, step), step))
            return carry

        lax.fori_loop(0, rows // step, once, 0)

    def loop(low, high, body):
        def once(i, carry):
            body(i)
            return carry

        lax.fori_loop(low, high, once, 0)

    def fetch_units(k):
        at = pl.ds(pl.multiple_of(k * tile, tile), tile)
        return pltpu.make_async_copy(hidden.at[:, at], units.at[:, at], fetch_sem.at[k])

    def fetch_cotangent(i, low, high):
        at = pl.ds(low * LANES, (high - low) * LANES)
        return pltpu.make_async_copy(upstream.at[:, at], cotangent.at[:, at], fetch_sem.at[chunks + i])

    def compute(at, places, loading=False):
        size = len(places) * LANES

        def once(k):
            if loading:
                fetch_units(k).wait()
            product = lax.dot_general(
                units[:, pl.ds(pl.multiple_of(k * tile, tile), tile)],
                cotangent[:, columns(at, size)],
                (((0,), (0,)), ((), ())),
                preferred_element_type=jnp.float32,
            ).reshape(blocks, near, rows, size)
            to = pl.ds(k * blocks, blocks)
            for i, (kind, index) in enumerate(places):
                piece = product[:, :, :, i * LANES : (i + 1) * LANES]
                if kind == "first":
                    first_own[index, to] = piece.astype(LINKED)
                else:
                    own[index, to] = jnp.where(y == 0, piece[:, 0], piece[:, 1]).astype(LINKED)
                    away[index % RING, to] = jnp.where(y == 0, piece[:, 1], piece[:, 0]).astype(LINKED)

        loop(0, chunks, once)

    def line(t, edge, middle, fill, up, down):
        up_b = far - 1 - t + z
        down_b = t - (far - 1) + z
        if edge:
            @pl.when(z == 0)
            def _():
                fill(up_b, False)
                up(t, up_b).start()

            @pl.when(z == far - 1)
            def _():
                fill(down_b, False)
                down(t, down_b).start()

        if middle:
            @pl.when((z > 0) & (z <= t) & (z < far - 1))
            def _():
                up(t - 1, up_b).wait_recv()
                fill(up_b, True)
                up(t, up_b).start()

            @pl.when((z < far - 1) & (z >= far - 1 - t) & (z > 0))
            def _():
                down(t - 1, down_b).wait_recv()
                fill(down_b, True)
                down(t, down_b).start()

    def term(c, h, b):
        return wide(own[c, b, part(h), :]) + wide(came[c, b, part(h), :])

    def line_step(c, h, t, edge, middle):
        def fill(b, add):
            value = term(c, h, b)
            if add:
                value = value + wide(slots[c, b, part(h), :])
            slots[c, b, part(h), :] = value.astype(LINKED)

        line(t, edge, middle, fill, lambda t, b: up_copy(c, h, t, b), lambda t, b: down_copy(c, h, t, b))

    def first_step(j, t, edge, middle):
        def fill(b, add):
            for side in range(near):
                def body(r):
                    value = first_own[j, b, side, r, :]
                    if add:
                        value = (wide(value) + wide(first_slots[j, b, side, r, :])).astype(LINKED)
                    first_slots[j, b, side, r, :] = value

                each_rows(body)

        line(t, edge, middle, fill, lambda t, b: first_up_copy(j, t, b), lambda t, b: first_down_copy(j, t, b))

    def settle(at, h, value):
        grad[part(h), columns(at)] = value.astype(LINKED)
        square = value * value
        total = square[0:8]
        for i in range(8, half, 8):
            total = total + square[i : i + 8]
        running[...] = running[...] + total
        for l in range(levels):
            grad_copy(at, h, l).start()

    def wait_own(up, down):
        @pl.when(z > 0)
        def _():
            up(far - 2, z).wait_recv()

        @pl.when(z < far - 1)
        def _():
            down(far - 2, far).wait_recv()

    def finish(c, h):
        wait_own(lambda t, b: up_copy(c, h, t, b), lambda t, b: down_copy(c, h, t, b))
        value = term(c, h, z)
        value = value + jnp.where(z > 0, wide(slots[c, z, part(h), :]), 0.0)
        value = value + jnp.where(z < far - 1, wide(slots[c, far, part(h), :]), 0.0)
        settle(first + c, h, value)

    def finish_first(j):
        wait_own(lambda t, b: first_up_copy(j, t, b), lambda t, b: first_down_copy(j, t, b))

        def put(r):
            def own_value(side):
                value = wide(first_own[j, z, side, r, :])
                value = value + jnp.where(z > 0, wide(first_slots[j, z, side, r, :]), 0.0)
                return value + jnp.where(z < far - 1, wide(first_slots[j, far, side, r, :]), 0.0)

            turn_own[j, r, :] = own_value(y)
            turn_out[j, r, :] = own_value(near - 1 - y).astype(LINKED)

        each_rows(put)
        turn_copy(j).start()

    def finish_turn(j):
        turn_copy(j).wait()
        for h in range(splits):
            settle(first - 1 - j, h, turn_own[j, part(h), :] + wide(turn_in[j, part(h), :]))

    steps = first * (far - 1)
    span = max(1, pieces - 3)

    def reached(c):
        goal = START + lax.div((c + 1) * (steps - START), span)
        return jnp.where(c < 0, START, jnp.minimum(steps, goal))

    def crossed(c):
        return jnp.where(c < LAG, 0, reached(c - LAG))

    def when(condition, body):
        pl.when(condition)(body)

    lead = (first - 1, first + 1)
    fetch_cotangent(0, *lead).start()
    loop(0, chunks, lambda k: fetch_units(k).start())
    fetch_cotangent(1, lead[1], first + pieces).start()
    fetch_cotangent(2, 0, lead[0]).start()
    running[...] = jnp.zeros((8, LANES), jnp.float32)
    weights[0] = weight[...]
    fetch_cotangent(0, *lead).wait()
    compute(first - 1, [("first", 0), ("near", 0)], loading=True)
    pl.semaphore_wait(barrier, len(receivers))
    near_copy(0, 0).start()
    first_step(0, 0, True, False)
    fetch_cotangent(1, lead[1], first + pieces).wait()
    fetch_cotangent(2, 0, lead[0]).wait()
    compute(first + 1, [("near", c) for c in range(1, AHEAD)])
    for k in range(1, FLIGHT):
        near_copy(k // splits, k % splits).start()
    compute(0, [("first", j) for j in range(first - 1, 0, -1)])

    for q in range(1, START):
        first_step(q // (far - 1), q % (far - 1), True, False)

    def stage_copy(i):
        return pltpu.make_async_copy(
            state.at[pl.ds(pl.multiple_of(i * chunk_rows, chunk_rows), chunk_rows)], stage.at[i % 2], stage_sem.at[i % 2]
        )

    stage_copy(0).start()

    def cast_rows(i):
        stage_copy(i).wait()
        when(i + 1 < rows // chunk_rows, lambda: stage_copy(i + 1).start())
        cast[pl.ds(pl.multiple_of(i * chunk_rows, chunk_rows), chunk_rows), :] = stage[i % 2].astype(LINKED)

    loop(0, rows // chunk_rows, cast_rows)
    for l in range(levels):
        state_copy(l).start()
        weight_copy(l).start()

    def prepare(c):
        for h in range(splits):
            when(c >= RING, lambda: near_copy(c - RING, h).wait_send())
        compute(first + c, [("near", c)])

    def drain_line(t, up, down):
        @pl.when((z <= t) & (z < far - 1))
        def _():
            up(t, far - 1 - t + z).wait_send()

        @pl.when((z >= far - 1 - t) & (z > 0))
        def _():
            down(t, t - (far - 1) + z).wait_send()

    def drain(c, h):
        when(c >= pieces - RING, lambda: near_copy(c, h).wait_send())
        loop(0, far - 1, lambda t: drain_line(
            t, lambda t, b: up_copy(c, h, t, b), lambda t, b: down_copy(c, h, t, b)))

    total_pieces = pieces * splits

    def piece(k, body):
        when((k >= 0) & (k < total_pieces), lambda: body(lax.div(k, splits), lax.rem(k, splits)))

    def tick(k):
        piece(k - MIDDLE * (far - 1), finish)

        def middle_step(i):
            t = far - 2 - i
            piece(k - MIDDLE * t, lambda c, h: line_step(c, h, t, False, True))

        def edge_step(i):
            t = far - 2 - i
            piece(k - EDGE * t, lambda c, h: line_step(c, h, t, True, False))

        def newest(c, h):
            near_copy(c, h).wait_recv()
            piece(k + FLIGHT, lambda c, h: near_copy(c, h).start())
            line_step(c, h, 0, True, False)

        loop(0, far - 2, middle_step)
        loop(0, far - 2, edge_step)
        piece(k, newest)
        c = lax.div(k, splits)

        @pl.when(lax.rem(k, splits) == 0)
        def _():
            when(c + AHEAD < pieces, lambda: prepare(c + AHEAD))

        @pl.when(lax.rem(k, splits) == splits - 1)
        def _():
            loop(lax.div(crossed(c - 2), far - 1), lax.div(crossed(c - 1), far - 1), finish_turn)
            loop(lax.div(crossed(c - 1), far - 1), lax.div(crossed(c), far - 1), finish_first)

            def first_edge(q):
                first_step(lax.div(q, far - 1), lax.rem(q, far - 1), True, False)

            def first_middle(q):
                first_step(lax.div(q, far - 1), lax.rem(q, far - 1), False, True)

            loop(reached(c - 1), reached(c), first_edge)
            loop(crossed(c), crossed(c + 1), first_middle)

        piece(k - DRAIN, drain)

    loop(0, total_pieces + MIDDLE * (far - 1), tick)

    def norm_copy(l, s_from, e):
        d = 0 if l == 0 else offsets[l - 1]
        at = norms.at[l, s_from]
        return remote(summed, at, norm_send.at[l, e], norm_recv.at[l, e], ((g + d) % groups, (s + e) % count))

    summed[...] = jnp.sum(running[...], axis=0, keepdims=True)
    messages = [(l, e) for l in range(levels + 1) for e in range(count) if l or e]
    for l, e in messages:
        norm_copy(l, s, e).start()
    norms[0, s] = summed[...]

    def drain_first(j):
        loop(0, far - 1, lambda t: drain_line(
            t, lambda t, b: first_up_copy(j, t, b), lambda t, b: first_down_copy(j, t, b)))

    def drain_grads(at):
        for h in range(splits):
            for l in range(levels):
                grad_copy(at, h, l).wait()

    for l in range(levels):
        state_copy(l).wait()
        weight_copy(l).wait()
    loop(0, first, drain_first)
    loop(max(0, total_pieces + MIDDLE * (far - 1) - DRAIN), total_pieces, lambda k: piece(k, drain))
    loop(0, first + pieces, drain_grads)
    for l, e in messages:
        norm_copy(l, (s + count - e) % count, e).wait_recv()
    for l in range(levels + 1):
        total = norms[l, 0]
        for d in range(1, count):
            total = total + norms[l, d]
        totals[l, 0] = total
        totals[l, 1] = weights[l]
    for l, e in messages:
        norm_copy(l, s, e).wait_send()


def reduced(hidden, upstream, state, weight, plan):
    far, near, rows, first, pieces, splits = (plan[k] for k in ("far", "near", "rows", "first", "pieces", "splits"))
    levels, count, width = len(plan["offsets"]), far * near, state.shape[1]
    anywhere, vmem = pl.BlockSpec(memory_space=pl.ANY), pl.BlockSpec(memory_space=pltpu.VMEM)
    dma, single = pltpu.SemaphoreType.DMA, jnp.float32
    scratch = [
        pltpu.VMEM(hidden.shape, LINKED),
        pltpu.VMEM(upstream.shape, LINKED),
        pltpu.VMEM((pieces, far, rows, LANES), LINKED),
        pltpu.VMEM((RING, far, rows, LANES), LINKED),
        pltpu.VMEM((pieces, far, rows, LANES), LINKED),
        pltpu.VMEM((pieces, far + 1, rows, LANES), LINKED),
        pltpu.VMEM((first, far, near, rows, LANES), LINKED),
        pltpu.VMEM((first, far + 1, near, rows, LANES), LINKED),
        pltpu.VMEM((first, rows, LANES), single),
        pltpu.VMEM((first, rows, LANES), LINKED),
        pltpu.VMEM((first, rows, LANES), LINKED),
        pltpu.VMEM((rows, width), LINKED),
        pltpu.VMEM((2, step_of_rows(rows), width), single),
        pltpu.VMEM((8, LANES), single),
        pltpu.VMEM((1, LANES), single),
        pltpu.VMEM((levels + 1, 1, LANES), single),
        pltpu.VMEM((levels + 1, count, 1, LANES), single),
        dma((far * near * rows // plan["tile"] + 3,)),
        dma((2,)),
    ]
    scratch += [dma((pieces, splits))] * 2 + [dma((pieces, splits, far - 1))] * 4 + [dma((first, far - 1))] * 4
    scratch += [dma((first,))] * 2 + [dma((levels,))] * 2 + [dma((first + pieces, splits, levels))] * 2
    scratch += [dma((levels + 1, count))] * 2 + [dma((levels,))] * 2
    peers = jax.ShapeDtypeStruct((levels, rows, width), LINKED)
    return pl.pallas_call(
        functools.partial(kernel, plan),
        out_shape=[
            jax.ShapeDtypeStruct((rows, width), LINKED),
            jax.ShapeDtypeStruct((levels + 1, 2, 1, LANES), single),
            peers,
            peers,
        ],
        in_specs=[anywhere] * 3 + [vmem],
        out_specs=[vmem, vmem, anywhere, anywhere],
        scratch_shapes=scratch,
        compiler_params=pltpu.CompilerParams(
            collective_id=0, has_side_effects=True, vmem_limit_bytes=63 * 1024 * 1024
        ),
    )(hidden, upstream, state, weight)


def update(levels, entry_count, step, totals, state, grad, peer_state, peer_grad, mixed_out, params_out, weight_out, held):
    @pl.when(pl.program_id(0) == 0)
    def _():
        bit = lax.rem(step[0], levels)
        when = jnp.full((1, LANES), step[0], jnp.int32).astype(jnp.float32)
        rate = learning_rate / jnp.sqrt(1.0 + when / decay_steps)

        def factor(l):
            squares = jnp.sum(totals[l, 0], keepdims=True)
            return rate * jnp.minimum(1.0, clip_ceiling / jnp.sqrt(squares / entry_count + epsilon))

        weight_next = 0.5 * (totals[0, 1] + totals[1 + bit, 1])
        weight_out[0] = jnp.max(weight_next)
        held[0] = 0.5 * factor(0)
        held[1] = 0.5 * factor(1 + bit)
        held[2] = 1.0 / weight_next

    mine, other, scale = (held[i, 0:1, 0:1] for i in range(3))
    mixed = 0.5 * (state[...] + wide(peer_state[0])) - (mine * wide(grad[...]) + other * wide(peer_grad[0]))
    mixed_out[...] = mixed
    params_out[...] = (mixed * scale).astype(jnp.bfloat16)


def updated(step_index, totals, state, grad, peer_states, peer_grads, entry_count):
    levels, (rows, width) = peer_states.shape[0], state.shape
    step = next(t for t in (UPDATE, step_of_rows(rows)) if rows % t == 0)
    here = pl.BlockSpec((step, width), lambda i, at: (i, 0))
    chosen = pl.BlockSpec((1, step, width), lambda i, at: (lax.rem(at[0], levels), i, 0))
    return pl.pallas_call(
        functools.partial(update, levels, entry_count),
        out_shape=[
            jax.ShapeDtypeStruct((rows, width), jnp.float32),
            jax.ShapeDtypeStruct((rows, width), jnp.bfloat16),
            jax.ShapeDtypeStruct((1,), jnp.float32),
        ],
        grid_spec=pltpu.PrefetchScalarGridSpec(
            num_scalar_prefetch=1,
            grid=(rows // step,),
            in_specs=[pl.BlockSpec(totals.shape, lambda i, at: (0, 0, 0, 0)), here, here, chosen, chosen],
            out_specs=[here, here, pl.BlockSpec(memory_space=pltpu.SMEM)],
            scratch_shapes=[pltpu.VMEM((3, 1, LANES), jnp.float32)],
        ),
    )(step_index, totals, state, grad, peer_states, peer_grads)


def shards(step_index, hidden, upstream, numerator, push_weight):
    own_state = numerator[0]
    groups = lax.axis_size("group")
    count = lax.axis_size("shard")
    level_count = groups.bit_length() - 1
    rows, width = own_state.shape
    units = rows * count
    tiles = width // LANES
    first = max(1, tiles // 6)
    plan = {
        "groups": groups,
        "far": count // NEAR,
        "near": NEAR,
        "rows": rows,
        "first": first,
        "pieces": tiles - first,
        "splits": 2 if rows % 32 == 0 else 1,
        "tile": next(t for t in (1152, units) if units % t == 0 and t % (NEAR * rows) == 0),
        "offsets": tuple(1 << bit for bit in range(level_count)),
    }
    weight = jnp.broadcast_to(push_weight[0], (1, LANES))
    gradient, totals, peer_states, peer_grads = reduced(hidden[0], upstream[0], own_state, weight, plan)
    mixed_state, new_params, weight_next = updated(
        step_index, totals, own_state, gradient, peer_states, peer_grads, units * width
    )
    return (mixed_state[None], weight_next, new_params[None])


def solution(mesh):
    placed = (
        P(),
        P("group", "shard", None),
        P("group", "shard", None),
        P("group", "shard", None),
        P("group"),
    )
    return jax.shard_map(
        shards,
        mesh=mesh,
        in_specs=placed,
        out_specs=(P("group", "shard", None), P("group"), P("group", "shard", None)),
        check_vma=False,
    )
```

```python
import functools

import jax
import jax.numpy as jnp
from jax import lax
from jax.experimental import pallas as pl
from jax.experimental.pallas import tpu as pltpu
from jax.sharding import PartitionSpec as P

learning_rate = 0.3
decay_steps = 256.0
clip_ceiling = 1.0
epsilon = 1e-06
LANES = 128
LINKED = jnp.bfloat16
MESH = pl.DeviceIdType.MESH
NEAR = 2
AHEAD = 3
RING = 4
FLIGHT = 2
EDGE = 1
MIDDLE = 2
START = 2
LAG = 1
DRAIN = 10
UPDATE = 144


def wide(x):
    return x.astype(jnp.float32)


def step_of_rows(rows):
    for step in (96, 64, 48, 32, 16):
        if rows % step == 0:
            return step
    return rows


def kernel(plan, hidden, upstream, state, weight, grad, totals, peer_states, peer_grads, *refs):
    groups, far, near, rows, offsets = (plan[k] for k in ("groups", "far", "near", "rows", "offsets"))
    first, pieces, splits, tile = (plan[k] for k in ("first", "pieces", "splits", "tile"))
    levels, count, half = len(offsets), far * near, rows // splits
    (units, cotangent, own, away, came, slots, first_own, first_slots, turn_own, turn_out, turn_in, cast, stage,
     running, summed, weights, norms, fetch_sem, stage_sem, near_send, near_recv, up_send, up_recv, down_send, down_recv,
     first_up_send, first_up_recv, first_down_send, first_down_recv, turn_send, turn_recv, state_send, state_recv,
     grad_send, grad_recv, norm_send, norm_recv, weight_send, weight_recv, lead_send, lead_recv) = refs

    g, s = lax.axis_index("group"), lax.axis_index("shard")
    z, y = s // near, s % near
    near_peer = (g, z * near + (near - 1 - y))
    above = (g, (s + near) % count)
    below = (g, (s + count - near) % count)
    chunks, blocks = far * near * rows // tile, tile // (near * rows)
    chunk_rows = stage.shape[1]

    receivers = [(0, d) for d in range(1, count)]
    receivers += [(d, e) for d in range(1, groups) for e in range(count)]
    barrier = pltpu.get_barrier_semaphore()
    for d, e in receivers:
        pl.semaphore_signal(barrier, inc=1, device_id=((g + d) % groups, (s + e) % count), device_id_type=MESH)

    def remote(src, dst, send, recv, device):
        return pltpu.make_async_remote_copy(
            src_ref=src, dst_ref=dst, send_sem=send, recv_sem=recv, device_id=device, device_id_type=MESH
        )

    def part(h):
        return pl.ds(h * half if isinstance(h, int) else pl.multiple_of(h * half, half), half)

    def columns(at, size=LANES):
        return pl.ds(pl.multiple_of(at * LANES, LANES), size)

    def near_copy(c, h):
        return remote(
            away.at[c % RING, :, part(h)], came.at[c, :, part(h)], near_send.at[c, h], near_recv.at[c, h], near_peer
        )

    def lead_copy(k):
        to = pl.ds(k * blocks, blocks)
        return remote(away.at[0, to], came.at[0, to], lead_send.at[k], lead_recv.at[k], near_peer)

    def up_copy(c, h, t, b):
        at = slots.at[c, b, part(h)]
        return remote(at, at, up_send.at[c, h, t], up_recv.at[c, h, t], above)

    def down_copy(c, h, t, b):
        to = jnp.where(t == far - 2, far, b)
        return remote(
            slots.at[c, b, part(h)], slots.at[c, to, part(h)], down_send.at[c, h, t], down_recv.at[c, h, t], below
        )

    def first_up_copy(j, t, b):
        at = first_slots.at[j, b]
        return remote(at, at, first_up_send.at[j, t], first_up_recv.at[j, t], above)

    def first_down_copy(j, t, b):
        to = jnp.where(t == far - 2, far, b)
        return remote(
            first_slots.at[j, b], first_slots.at[j, to], first_down_send.at[j, t], first_down_recv.at[j, t], below
        )

    def turn_copy(j):
        return remote(turn_out.at[j], turn_in.at[j], turn_send.at[j], turn_recv.at[j], near_peer)

    def state_copy(l):
        return remote(cast, peer_states.at[l], state_send.at[l], state_recv.at[l], ((g + offsets[l]) % groups, s))

    def weight_copy(l):
        to = weights.at[l + 1]
        return remote(weight, to, weight_send.at[l], weight_recv.at[l], ((g + offsets[l]) % groups, s))

    def grad_copy(at, h, l):
        return remote(
            grad.at[part(h), columns(at)],
            peer_grads.at[l, part(h), columns(at)],
            grad_send.at[at, h, l],
            grad_recv.at[at, h, l],
            ((g + offsets[l]) % groups, s),
        )

    def each_rows(body):
        step = step_of_rows(rows)

        def once(i, carry):
            body(pl.ds(pl.multiple_of(i * step, step), step))
            return carry

        lax.fori_loop(0, rows // step, once, 0)

    def loop(low, high, body):
        def once(i, carry):
            body(i)
            return carry

        lax.fori_loop(low, high, once, 0)

    def fetch_units(k):
        at = pl.ds(pl.multiple_of(k * tile, tile), tile)
        return pltpu.make_async_copy(hidden.at[:, at], units.at[:, at], fetch_sem.at[k])

    def fetch_cotangent(i, low, high):
        at = pl.ds(low * LANES, (high - low) * LANES)
        return pltpu.make_async_copy(upstream.at[:, at], cotangent.at[:, at], fetch_sem.at[chunks + i])

    def compute(at, places, after=None):
        size = len(places) * LANES

        def once(k):
            if after:
                fetch_units(k).wait()
            product = lax.dot_general(
                units[:, pl.ds(pl.multiple_of(k * tile, tile), tile)],
                cotangent[:, columns(at, size)],
                (((0,), (0,)), ((), ())),
                preferred_element_type=jnp.float32,
            ).reshape(blocks, near, rows, size)
            to = pl.ds(k * blocks, blocks)
            for i, (kind, index) in enumerate(places):
                piece = product[:, :, :, i * LANES : (i + 1) * LANES]
                if kind == "first":
                    first_own[index, to] = piece.astype(LINKED)
                else:
                    own[index, to] = jnp.where(y == 0, piece[:, 0], piece[:, 1]).astype(LINKED)
                    away[index % RING, to] = jnp.where(y == 0, piece[:, 1], piece[:, 0]).astype(LINKED)

            if after:
                after(k)

        loop(0, chunks, once)

    def line(t, edge, middle, fill, up, down):
        up_b = far - 1 - t + z
        down_b = t - (far - 1) + z
        if edge:
            @pl.when(z == 0)
            def _():
                fill(up_b, False)
                up(t, up_b).start()

            @pl.when(z == far - 1)
            def _():
                fill(down_b, False)
                down(t, down_b).start()

        if middle:
            @pl.when((z > 0) & (z <= t) & (z < far - 1))
            def _():
                up(t - 1, up_b).wait_recv()
                fill(up_b, True)
                up(t, up_b).start()

            @pl.when((z < far - 1) & (z >= far - 1 - t) & (z > 0))
            def _():
                down(t - 1, down_b).wait_recv()
                fill(down_b, True)
                down(t, down_b).start()

    def term(c, h, b):
        return wide(own[c, b, part(h), :]) + wide(came[c, b, part(h), :])

    def line_step(c, h, t, edge, middle):
        def fill(b, add):
            value = term(c, h, b)
            if add:
                value = value + wide(slots[c, b, part(h), :])
            slots[c, b, part(h), :] = value.astype(LINKED)

        line(t, edge, middle, fill, lambda t, b: up_copy(c, h, t, b), lambda t, b: down_copy(c, h, t, b))

    def first_step(j, t, edge, middle):
        def fill(b, add):
            for side in range(near):
                def body(r):
                    value = first_own[j, b, side, r, :]
                    if add:
                        value = (wide(value) + wide(first_slots[j, b, side, r, :])).astype(LINKED)
                    first_slots[j, b, side, r, :] = value

                each_rows(body)

        line(t, edge, middle, fill, lambda t, b: first_up_copy(j, t, b), lambda t, b: first_down_copy(j, t, b))

    def settle(at, h, value):
        grad[part(h), columns(at)] = value.astype(LINKED)
        square = value * value
        total = square[0:8]
        for i in range(8, half, 8):
            total = total + square[i : i + 8]
        running[...] = running[...] + total
        for l in range(levels):
            grad_copy(at, h, l).start()

    def wait_own(up, down):
        @pl.when(z > 0)
        def _():
            up(far - 2, z).wait_recv()

        @pl.when(z < far - 1)
        def _():
            down(far - 2, far).wait_recv()

    def finish(c, h):
        wait_own(lambda t, b: up_copy(c, h, t, b), lambda t, b: down_copy(c, h, t, b))
        value = term(c, h, z)
        value = value + jnp.where(z > 0, wide(slots[c, z, part(h), :]), 0.0)
        value = value + jnp.where(z < far - 1, wide(slots[c, far, part(h), :]), 0.0)
        settle(first + c, h, value)

    def finish_first(j):
        wait_own(lambda t, b: first_up_copy(j, t, b), lambda t, b: first_down_copy(j, t, b))

        def put(r):
            def own_value(side):
                value = wide(first_own[j, z, side, r, :])
                value = value + jnp.where(z > 0, wide(first_slots[j, z, side, r, :]), 0.0)
                return value + jnp.where(z < far - 1, wide(first_slots[j, far, side, r, :]), 0.0)

            turn_own[j, r, :] = own_value(y)
            turn_out[j, r, :] = own_value(near - 1 - y).astype(LINKED)

        each_rows(put)
        turn_copy(j).start()

    def finish_turn(j):
        turn_copy(j).wait()
        for h in range(splits):
            settle(first - 1 - j, h, turn_own[j, part(h), :] + wide(turn_in[j, part(h), :]))

    steps = first * (far - 1)
    span = max(1, pieces - 3)

    def reached(c):
        goal = START + lax.div((c + 1) * (steps - START), span)
        return jnp.where(c < 0, START, jnp.minimum(steps, goal))

    def crossed(c):
        return jnp.where(c < LAG, 0, reached(c - LAG))

    def when(condition, body):
        pl.when(condition)(body)

    lead = (first - 1, first + 1)
    fetch_cotangent(0, *lead).start()
    loop(0, chunks, lambda k: fetch_units(k).start())
    fetch_cotangent(1, lead[1], first + pieces).start()
    fetch_cotangent(2, 0, lead[0]).start()
    running[...] = jnp.zeros((8, LANES), jnp.float32)
    weights[0] = weight[...]
    fetch_cotangent(0, *lead).wait()

    def after(k):
        when(k == 0, lambda: pl.semaphore_wait(barrier, len(receivers)))
        lead_copy(k).start()

    compute(first - 1, [("first", 0), ("near", 0)], after)
    first_step(0, 0, True, False)
    fetch_cotangent(1, lead[1], first + pieces).wait()
    fetch_cotangent(2, 0, lead[0]).wait()
    compute(first + 1, [("near", c) for c in range(1, AHEAD)])
    near_copy(1, 0).start()
    compute(0, [("first", j) for j in range(first - 1, 0, -1)])

    for q in range(1, START):
        first_step(q // (far - 1), q % (far - 1), True, False)

    def stage_copy(i):
        return pltpu.make_async_copy(
            state.at[pl.ds(pl.multiple_of(i * chunk_rows, chunk_rows), chunk_rows)], stage.at[i % 2], stage_sem.at[i % 2]
        )

    stage_copy(0).start()

    def cast_rows(i):
        stage_copy(i).wait()
        when(i + 1 < rows // chunk_rows, lambda: stage_copy(i + 1).start())
        cast[pl.ds(pl.multiple_of(i * chunk_rows, chunk_rows), chunk_rows), :] = stage[i % 2].astype(LINKED)

    loop(0, rows // chunk_rows, cast_rows)
    for l in range(levels):
        state_copy(l).start()
        weight_copy(l).start()

    def prepare(c):
        when(c == RING, lambda: loop(0, chunks, lambda k: lead_copy(k).wait_send()))
        for h in range(splits):
            when(c > RING, lambda: near_copy(c - RING, h).wait_send())
        compute(first + c, [("near", c)])

    def drain_line(t, up, down):
        @pl.when((z <= t) & (z < far - 1))
        def _():
            up(t, far - 1 - t + z).wait_send()

        @pl.when((z >= far - 1 - t) & (z > 0))
        def _():
            down(t, t - (far - 1) + z).wait_send()

    def drain(c, h):
        when(c >= pieces - RING, lambda: near_copy(c, h).wait_send())
        loop(0, far - 1, lambda t: drain_line(
            t, lambda t, b: up_copy(c, h, t, b), lambda t, b: down_copy(c, h, t, b)))

    total_pieces = pieces * splits

    def piece(k, body):
        when((k >= 0) & (k < total_pieces), lambda: body(lax.div(k, splits), lax.rem(k, splits)))

    def tick(k):
        piece(k - MIDDLE * (far - 1), finish)

        def middle_step(i):
            t = far - 2 - i
            piece(k - MIDDLE * t, lambda c, h: line_step(c, h, t, False, True))

        def edge_step(i):
            t = far - 2 - i
            piece(k - EDGE * t, lambda c, h: line_step(c, h, t, True, False))

        def newest(c, h):
            when(c == 0, lambda: when(h == 0, lambda: loop(0, chunks, lambda k: lead_copy(k).wait_recv())))
            when(c > 0, lambda: near_copy(c, h).wait_recv())
            when(k + FLIGHT > splits, lambda: piece(k + FLIGHT, lambda c, h: near_copy(c, h).start()))
            line_step(c, h, 0, True, False)

        loop(0, far - 2, middle_step)
        loop(0, far - 2, edge_step)
        piece(k, newest)
        c = lax.div(k, splits)

        @pl.when(lax.rem(k, splits) == 0)
        def _():
            when(c + AHEAD < pieces, lambda: prepare(c + AHEAD))

        @pl.when(lax.rem(k, splits) == splits - 1)
        def _():
            loop(lax.div(crossed(c - 2), far - 1), lax.div(crossed(c - 1), far - 1), finish_turn)
            loop(lax.div(crossed(c - 1), far - 1), lax.div(crossed(c), far - 1), finish_first)

            def first_edge(q):
                first_step(lax.div(q, far - 1), lax.rem(q, far - 1), True, False)

            def first_middle(q):
                first_step(lax.div(q, far - 1), lax.rem(q, far - 1), False, True)

            loop(reached(c - 1), reached(c), first_edge)
            loop(crossed(c), crossed(c + 1), first_middle)

        piece(k - DRAIN, drain)

    loop(0, total_pieces + MIDDLE * (far - 1), tick)

    def norm_copy(l, s_from, e):
        d = 0 if l == 0 else offsets[l - 1]
        at = norms.at[l, s_from]
        return remote(summed, at, norm_send.at[l, e], norm_recv.at[l, e], ((g + d) % groups, (s + e) % count))

    summed[...] = jnp.sum(running[...], axis=0, keepdims=True)
    messages = [(l, e) for l in range(levels + 1) for e in range(count) if l or e]
    for l, e in messages:
        norm_copy(l, s, e).start()
    norms[0, s] = summed[...]

    def drain_first(j):
        loop(0, far - 1, lambda t: drain_line(
            t, lambda t, b: first_up_copy(j, t, b), lambda t, b: first_down_copy(j, t, b)))

    def drain_grads(at):
        for h in range(splits):
            for l in range(levels):
                grad_copy(at, h, l).wait()

    for l in range(levels):
        state_copy(l).wait()
        weight_copy(l).wait()
    loop(0, first, drain_first)
    loop(max(0, total_pieces + MIDDLE * (far - 1) - DRAIN), total_pieces, lambda k: piece(k, drain))
    loop(0, first + pieces, drain_grads)
    for l, e in messages:
        norm_copy(l, (s + count - e) % count, e).wait_recv()
    for l in range(levels + 1):
        total = norms[l, 0]
        for d in range(1, count):
            total = total + norms[l, d]
        totals[l, 0] = total
        totals[l, 1] = weights[l]
    for l, e in messages:
        norm_copy(l, s, e).wait_send()


def reduced(hidden, upstream, state, weight, plan):
    far, near, rows, first, pieces, splits = (plan[k] for k in ("far", "near", "rows", "first", "pieces", "splits"))
    levels, count, width = len(plan["offsets"]), far * near, state.shape[1]
    anywhere, vmem = pl.BlockSpec(memory_space=pl.ANY), pl.BlockSpec(memory_space=pltpu.VMEM)
    dma, single = pltpu.SemaphoreType.DMA, jnp.float32
    scratch = [
        pltpu.VMEM(hidden.shape, LINKED),
        pltpu.VMEM(upstream.shape, LINKED),
        pltpu.VMEM((pieces, far, rows, LANES), LINKED),
        pltpu.VMEM((RING, far, rows, LANES), LINKED),
        pltpu.VMEM((pieces, far, rows, LANES), LINKED),
        pltpu.VMEM((pieces, far + 1, rows, LANES), LINKED),
        pltpu.VMEM((first, far, near, rows, LANES), LINKED),
        pltpu.VMEM((first, far + 1, near, rows, LANES), LINKED),
        pltpu.VMEM((first, rows, LANES), single),
        pltpu.VMEM((first, rows, LANES), LINKED),
        pltpu.VMEM((first, rows, LANES), LINKED),
        pltpu.VMEM((rows, width), LINKED),
        pltpu.VMEM((2, step_of_rows(rows), width), single),
        pltpu.VMEM((8, LANES), single),
        pltpu.VMEM((1, LANES), single),
        pltpu.VMEM((levels + 1, 1, LANES), single),
        pltpu.VMEM((levels + 1, count, 1, LANES), single),
        dma((far * near * rows // plan["tile"] + 3,)),
        dma((2,)),
    ]
    scratch += [dma((pieces, splits))] * 2 + [dma((pieces, splits, far - 1))] * 4 + [dma((first, far - 1))] * 4
    scratch += [dma((first,))] * 2 + [dma((levels,))] * 2 + [dma((first + pieces, splits, levels))] * 2
    scratch += [dma((levels + 1, count))] * 2 + [dma((levels,))] * 2
    scratch += [dma((far * near * rows // plan["tile"],))] * 2
    peers = jax.ShapeDtypeStruct((levels, rows, width), LINKED)
    return pl.pallas_call(
        functools.partial(kernel, plan),
        out_shape=[
            jax.ShapeDtypeStruct((rows, width), LINKED),
            jax.ShapeDtypeStruct((levels + 1, 2, 1, LANES), single),
            peers,
            peers,
        ],
        in_specs=[anywhere] * 3 + [vmem],
        out_specs=[vmem, vmem, anywhere, anywhere],
        scratch_shapes=scratch,
        compiler_params=pltpu.CompilerParams(
            collective_id=0, has_side_effects=True, vmem_limit_bytes=63 * 1024 * 1024
        ),
    )(hidden, upstream, state, weight)


def update(levels, entry_count, step, totals, state, grad, peer_state, peer_grad, mixed_out, params_out, weight_out, held):
    @pl.when(pl.program_id(0) == 0)
    def _():
        bit = lax.rem(step[0], levels)
        when = jnp.full((1, LANES), step[0], jnp.int32).astype(jnp.float32)
        rate = learning_rate / jnp.sqrt(1.0 + when / decay_steps)

        def factor(l):
            squares = jnp.sum(totals[l, 0], keepdims=True)
            return rate * jnp.minimum(1.0, clip_ceiling / jnp.sqrt(squares / entry_count + epsilon))

        weight_next = 0.5 * (totals[0, 1] + totals[1 + bit, 1])
        weight_out[0] = jnp.max(weight_next)
        held[0] = 0.5 * factor(0)
        held[1] = 0.5 * factor(1 + bit)
        held[2] = 1.0 / weight_next

    mine, other, scale = (held[i, 0:1, 0:1] for i in range(3))
    mixed = 0.5 * (state[...] + wide(peer_state[0])) - (mine * wide(grad[...]) + other * wide(peer_grad[0]))
    mixed_out[...] = mixed
    params_out[...] = (mixed * scale).astype(jnp.bfloat16)


def updated(step_index, totals, state, grad, peer_states, peer_grads, entry_count):
    levels, (rows, width) = peer_states.shape[0], state.shape
    step = next(t for t in (UPDATE, step_of_rows(rows)) if rows % t == 0)
    here = pl.BlockSpec((step, width), lambda i, at: (i, 0))
    chosen = pl.BlockSpec((1, step, width), lambda i, at: (lax.rem(at[0], levels), i, 0))
    return pl.pallas_call(
        functools.partial(update, levels, entry_count),
        out_shape=[
            jax.ShapeDtypeStruct((rows, width), jnp.float32),
            jax.ShapeDtypeStruct((rows, width), jnp.bfloat16),
            jax.ShapeDtypeStruct((1,), jnp.float32),
        ],
        grid_spec=pltpu.PrefetchScalarGridSpec(
            num_scalar_prefetch=1,
            grid=(rows // step,),
            in_specs=[pl.BlockSpec(totals.shape, lambda i, at: (0, 0, 0, 0)), here, here, chosen, chosen],
            out_specs=[here, here, pl.BlockSpec(memory_space=pltpu.SMEM)],
            scratch_shapes=[pltpu.VMEM((3, 1, LANES), jnp.float32)],
        ),
    )(step_index, totals, state, grad, peer_states, peer_grads)


def shards(step_index, hidden, upstream, numerator, push_weight):
    own_state = numerator[0]
    groups = lax.axis_size("group")
    count = lax.axis_size("shard")
    level_count = groups.bit_length() - 1
    rows, width = own_state.shape
    units = rows * count
    tiles = width // LANES
    first = max(1, tiles // 6)
    plan = {
        "groups": groups,
        "far": count // NEAR,
        "near": NEAR,
        "rows": rows,
        "first": first,
        "pieces": tiles - first,
        "splits": 2 if rows % 32 == 0 else 1,
        "tile": next(t for t in (1152, units) if units % t == 0 and t % (NEAR * rows) == 0),
        "offsets": tuple(1 << bit for bit in range(level_count)),
    }
    weight = jnp.broadcast_to(push_weight[0], (1, LANES))
    gradient, totals, peer_states, peer_grads = reduced(hidden[0], upstream[0], own_state, weight, plan)
    mixed_state, new_params, weight_next = updated(
        step_index, totals, own_state, gradient, peer_states, peer_grads, units * width
    )
    return (mixed_state[None], weight_next, new_params[None])


def solution(mesh):
    placed = (
        P(),
        P("group", "shard", None),
        P("group", "shard", None),
        P("group", "shard", None),
        P("group"),
    )
    return jax.shard_map(
        shards,
        mesh=mesh,
        in_specs=placed,
        out_specs=(P("group", "shard", None), P("group"), P("group", "shard", None)),
        check_vma=False,
    )
```
